32 devices in a mesh: rep: 2 (over x), dp: 16 (over y, z, core).
Axes of the slice: x: 2, y: 2, z: 4, core: 2. Of those that a mesh axis runs over, the one named last changes fastest.
Arguments:
- a: bfloat16 [32, 4, 4096, 1536], P(('rep', 'dp')), parts along dimension 0
- g: bfloat16 [32, 4, 4096, 4224], P(('rep', 'dp')), parts along dimension 0
Outputs:
- output: bfloat16 [8, 1536, 4224], P('rep'), parts along dimension 0
There are 2 independent parts. The reference program is written for one: setup_inputs(seed, part) draws one part's arguments, and reference() takes and returns one part's arrays. A program takes and returns all parts, laid end to end along the dimension named above; each array names one.
All inputs are finite; a program needn't handle non-finite values.
Results may differ from the reference program's by a relative error of at most 0.012.
Values are sent between devices in bfloat16 or wider.
A program may use at most 2 GiB of HBM per device.

```python
import jax
import jax.numpy as jnp
from jax import lax

DEVICES = 16
MATRICES = 4
TOKENS = 4096
D = 1536
FF = 4224


def setup_inputs(seed: int = 0, part: int = 0) -> dict:
    ka, kg, ks = (jax.random.fold_in(k, part) for k in jax.random.split(jax.random.key(seed), 3))
    size = 2.0 ** jax.random.uniform(ks, (DEVICES, MATRICES, 1, 1), jnp.float32, -1.0, 1.0)
    a = jax.random.normal(ka, (DEVICES, MATRICES, TOKENS, D), jnp.float32)
    g = size * jax.random.normal(kg, (DEVICES, MATRICES, TOKENS, FF), jnp.float32) * (DEVICES * TOKENS) ** -0.5
    return {"a": a.astype(jnp.bfloat16), "g": g.astype(jnp.bfloat16)}


def reference(a, g):
    def take(so_far, one):
        return so_far + jnp.einsum("ntd,ntf->ndf", *one, preferred_element_type=jnp.float32), None

    return lax.scan(take, jnp.zeros((MATRICES, D, FF), jnp.float32), (a, g))[0].astype(jnp.bfloat16)
```

```python
import functools

import jax
import jax.numpy as jnp
from jax import lax
from jax.experimental import pallas as pl
from jax.experimental.pallas import tpu as pltpu
from jax.sharding import PartitionSpec as P

MESH = pl.DeviceIdType.MESH
NM, TOK, D, FF = 4, 4096, 1536, 4224
HALF = D // 2
TM, TN, UM = 256, 1408, 128
TILES, SLICES = HALF // TM, FF // TN
CHUNKS = NM * SLICES * TILES
UPC = TM // UM
U = CHUNKS * UPC
STEPS = 2 * CHUNKS
GSTEPS = 2 * TILES
GROUPS = NM * SLICES
L0, LT = 1, 2
TOP = 8
OB = 16
RC = 8
BR = 24
TOTAL = STEPS + L0 + LT * TOP + 1
assert UPC == 2


def tree(u, y, z):
    pos, period = u % 10, u // 10
    third = pos // 3
    kind_b = (pos % 3 == 2) | (pos == 9)
    k = jnp.where(kind_b, third, 1 + (third + period) % 2)
    q = jnp.where(kind_b, (third + period) % 2, pos % 3)
    at_q = y == q
    on_line = kind_b | at_q
    at_k = z == k
    far = jnp.maximum(k, 3 - k)
    side = jnp.where(z < k, z, jnp.where(z > k, 3 - z, far))
    root = at_q & at_k
    height = jnp.where(
        kind_b, side + root.astype(jnp.int32), jnp.where(at_q, 1 + side, 0)
    )
    top = far + 1
    depth = jnp.abs(z - k) + (1 - at_q.astype(jnp.int32))
    child = (
        at_q & (at_k | ~kind_b),
        on_line & (z <= k) & (z > 0),
        on_line & (z >= k) & (z < 3),
    )
    parent = (
        ~at_q & (at_k | ~kind_b),
        on_line & (z > k),
        on_line & (z < k),
    )
    return height, top + depth, root, child, parent


def kernel(
    a_ref, g_ref, out_ref, box_ref,
    abuf, gbuf, sibout, own, outbox, stage,
    a_sem, g_sem, sib_send, recv, load, up_send, down_send, res, sibres,
):
    rep = lax.axis_index("rep")
    me = lax.axis_index("dp")
    core, z, y = me % 2, (me // 2) % 4, me // 8
    sib = (rep, me + 1 - 2 * core)
    near = (
        (rep, me + 8 - 16 * y),
        (rep, jnp.where(z > 0, me - 2, me + 2)),
        (rep, jnp.where(z < 3, me + 2, me - 2)),
    )

    def a_load(i):
        c = i // 2
        n, t = c // (SLICES * TILES), c % TILES
        half = jnp.where(i % 2 == 0, 1 - core, core)
        cols = pl.ds(pl.multiple_of(half * HALF + t * TM, 128), TM)
        return pltpu.make_async_copy(
            a_ref.at[0, n, :, cols], abuf.at[i % 2], a_sem.at[i % 2]
        )

    def g_load(gi):
        cols = pl.ds(pl.multiple_of((gi % SLICES) * TN, 128), TN)
        return pltpu.make_async_copy(
            g_ref.at[0, gi // SLICES, :, cols], gbuf.at[gi % 2], g_sem.at[gi % 2]
        )

    def remote(src, dst, send, rcv, device):
        return pltpu.make_async_remote_copy(
            src_ref=src, dst_ref=dst, send_sem=send, recv_sem=rcv,
            device_id=device, device_id_type=MESH,
        )

    def place(u):
        c = u // UPC
        n, s, t = c // (SLICES * TILES), (c // TILES) % SLICES, c % TILES
        row = pl.multiple_of(core * HALF + t * TM + (u % UPC) * UM, UM)
        col = pl.multiple_of(s * TN, 128)
        return out_ref.at[n, pl.ds(row, UM), pl.ds(col, TN)]

    def sib_copy(c, h):
        return remote(
            sibout.at[c % 2, pl.ds(h * UM, UM)], box_ref.at[c * UPC + h],
            sib_send.at[c % 2, h], recv.at[0, c * UPC + h], sib,
        )

    def up_copy(u, d):
        s = (1, 3, 2)[d]
        return remote(
            outbox.at[u % OB], box_ref.at[s * U + u], up_send.at[u % OB, 0],
            recv.at[s, u], near[d],
        )

    def root_copy(u, d):
        return remote(
            outbox.at[u % OB], place(u), up_send.at[u % OB, d],
            res.at[u], near[d],
        )

    def root_sib(u):
        return remote(
            outbox.at[u % OB], place(u), up_send.at[u % OB, 3], sibres.at[u], sib
        )

    def root_local(u):
        return pltpu.make_async_copy(
            outbox.at[u % OB], place(u), up_send.at[u % OB, 4]
        )

    def down_copy(u, d):
        return remote(place(u), place(u), down_send.at[u % BR, d], res.at[u], near[d])

    def down_sib(u):
        return remote(place(u), place(u), down_send.at[u % BR, 3], sibres.at[u], sib)

    def up_done(u):
        _, _, root, child, parent = tree(u, y, z)
        for d in range(3):
            @pl.when(parent[d])
            def _(d=d):
                up_copy(u, d).wait_send()

            @pl.when(root & child[d])
            def _(d=d):
                root_copy(u, d).wait_send()

        @pl.when(root)
        def _():
            root_sib(u).wait_send()
            root_local(u).wait()

    def down_done(u):
        _, _, root, child, _ = tree(u, y, z)
        for d in range(3):
            @pl.when(~root & child[d])
            def _(d=d):
                down_copy(u, d).wait_send()

        @pl.when(~root)
        def _():
            down_sib(u).wait_send()

    def stage_load(tau, u, s, slot):
        return pltpu.make_async_copy(
            box_ref.at[s * U + u], stage.at[tau, slot], load.at[tau, slot]
        )

    def gather(i):
        def one(tau, _):
            u = i - L0 - LT * tau
            ok = (u >= 0) & (u < U)
            uu = jnp.clip(u, 0, U - 1)
            height, _, _, child, _ = tree(uu, y, z)

            @pl.when(ok & (height == tau))
            def _():
                remote(box_ref.at[uu], box_ref.at[uu], sib_send.at[0, 0],
                       recv.at[0, uu], sib).wait_recv()
                stage_load(tau, uu, 0, 0).start()
                slot = jnp.int32(1)
                for d in range(3):
                    @pl.when(child[d])
                    def _(d=d, slot=slot):
                        b = box_ref.at[(d + 1) * U + uu]
                        remote(b, b, sib_send.at[0, 0], recv.at[d + 1, uu], sib).wait_recv()
                        stage_load(tau, uu, d + 1, slot).start()

                    slot = slot + child[d].astype(jnp.int32)

            return 0

        lax.fori_loop(0, 5, one, 0)

    def combine(i):
        def one(tau, _):
            u = i - L0 - LT * tau
            ok = (u >= 0) & (u < U)
            uu = jnp.clip(u, 0, U - 1)
            height, _, root, child, parent = tree(uu, y, z)
            count = sum(c.astype(jnp.int32) for c in child)

            @pl.when(ok & (height == tau))
            def _():
                @pl.when(uu >= OB)
                def _():
                    up_done(jnp.maximum(uu - OB, 0))

                for m in range(4):
                    @pl.when(count == m)
                    def _(m=m):
                        for slot in range(m + 1):
                            stage_load(tau, uu, 0, slot).wait()

                        def rows(r, _):
                            here = pl.ds(pl.multiple_of(r * 16, 16), 16)
                            there = pl.ds(
                                pl.multiple_of((uu % UPC) * UM + r * 16, 16), 16
                            )
                            acc = own[(uu // UPC) % RC, there, :]
                            for slot in range(m + 1):
                                acc = acc + stage[tau, slot, here, :].astype(jnp.float32)
                            outbox[uu % OB, here, :] = acc.astype(jnp.bfloat16)
                            return 0

                        lax.fori_loop(0, UM // 16, rows, 0)

                for d in range(3):
                    @pl.when(parent[d])
                    def _(d=d):
                        up_copy(uu, d).start()

                    @pl.when(root & child[d])
                    def _(d=d):
                        root_copy(uu, d).start()

                @pl.when(root)
                def _():
                    root_sib(uu).start()
                    root_local(uu).start()

            return 0

        lax.fori_loop(0, 5, one, 0)

    def forward(i):
        def one(tau, _):
            u = i - L0 - LT * tau
            ok = (u >= 0) & (u < U)
            uu = jnp.clip(u, 0, U - 1)
            _, when, root, child, _ = tree(uu, y, z)

            @pl.when(ok & (when == tau))
            def _():
                @pl.when(uu >= BR)
                def _():
                    down_done(jnp.maximum(uu - BR, 0))

                @pl.when(~root)
                def _():
                    remote(place(uu), place(uu), sib_send.at[0, 0], res.at[uu], sib).wait_recv()
                    for d in range(3):
                        @pl.when(child[d])
                        def _(d=d):
                            down_copy(uu, d).start()

                    down_sib(uu).start()

            return 0

        lax.fori_loop(3, TOP + 1, one, 0)

    def matmul(i):
        @pl.when(i % GSTEPS == 0)
        def _():
            g_load(i // GSTEPS).wait()

            @pl.when(i // GSTEPS + 1 < GROUPS)
            def _():
                g_load(i // GSTEPS + 1).start()

        a_load(i).wait()

        @pl.when(i + 1 < STEPS)
        def _():
            a_load(i + 1).start()

        c = i // 2

        def dot():
            return lax.dot_general(
                abuf[i % 2], gbuf[(i // GSTEPS) % 2], (((0,), (0,)), ((), ())),
                preferred_element_type=jnp.float32,
            )

        @pl.when(i % 2 == 0)
        def _():
            @pl.when(c >= 2)
            def _():
                for h in range(UPC):
                    sib_copy(jnp.maximum(c - 2, 0), h).wait_send()

            sibout[c % 2] = dot().astype(jnp.bfloat16)
            for h in range(UPC):
                sib_copy(c, h).start()

        @pl.when(i % 2 == 1)
        def _():
            own[c % RC] = dot()

    a_load(0).start()
    g_load(0).start()
    barrier = pltpu.get_barrier_semaphore()
    pl.semaphore_signal(barrier, inc=1, device_id=sib, device_id_type=MESH)
    pl.semaphore_signal(barrier, inc=1, device_id=near[0], device_id_type=MESH)

    @pl.when(z > 0)
    def _():
        pl.semaphore_signal(barrier, inc=1, device_id=near[1], device_id_type=MESH)

    @pl.when(z < 3)
    def _():
        pl.semaphore_signal(barrier, inc=1, device_id=near[2], device_id_type=MESH)

    inner = (z > 0) & (z < 3)

    @pl.when(inner)
    def _():
        pl.semaphore_wait(barrier, 4)

    @pl.when(~inner)
    def _():
        pl.semaphore_wait(barrier, 3)

    def step(i, _):
        forward(i)
        gather(i)

        @pl.when(i < STEPS)
        def _():
            matmul(i)

        combine(i)
        return 0

    lax.fori_loop(0, TOTAL, step, 0)

    for c in range(CHUNKS - 2, CHUNKS):
        for h in range(UPC):
            sib_copy(c, h).wait_send()

    def end_up(u, _):
        up_done(u)
        return 0

    lax.fori_loop(U - OB, U, end_up, 0)

    def end_down(u, _):
        down_done(u)
        return 0

    lax.fori_loop(U - BR, U, end_down, 0)

    def end_sib(u, _):
        c = u // UPC
        n, s, t = c // (SLICES * TILES), (c // TILES) % SLICES, c % TILES
        row = pl.multiple_of((1 - core) * HALF + t * TM + (u % UPC) * UM, UM)
        b = out_ref.at[n, pl.ds(row, UM), pl.ds(pl.multiple_of(s * TN, 128), TN)]
        remote(b, b, sib_send.at[0, 0], sibres.at[u], sib).wait_recv()
        return 0

    lax.fori_loop(0, U, end_sib, 0)


def solution(mesh):
    def body(a, g):
        dma = pltpu.SemaphoreType.DMA
        out, _ = pl.pallas_call(
            kernel,
            out_shape=[
                jax.ShapeDtypeStruct((NM, D, FF), jnp.bfloat16),
                jax.ShapeDtypeStruct((4 * U, UM, TN), jnp.bfloat16),
            ],
            in_specs=[pl.BlockSpec(memory_space=pl.ANY)] * 2,
            out_specs=[pl.BlockSpec(memory_space=pl.ANY)] * 2,
            scratch_shapes=[
                pltpu.VMEM((2, TOK, TM), jnp.bfloat16),
                pltpu.VMEM((2, TOK, TN), jnp.bfloat16),
                pltpu.VMEM((2, TM, TN), jnp.bfloat16),
                pltpu.VMEM((RC, TM, TN), jnp.float32),
                pltpu.VMEM((OB, UM, TN), jnp.bfloat16),
                pltpu.VMEM((5, 4, UM, TN), jnp.bfloat16),
                dma((2,)),
                dma((2,)),
                dma((2, UPC)),
                dma((4, U)),
                dma((5, 4)),
                dma((OB, 5)),
                dma((BR, 4)),
                dma((U,)),
                dma((U,)),
            ],
            compiler_params=pltpu.CompilerParams(
                collective_id=0, has_side_effects=True, vmem_limit_bytes=63 * 2**20
            ),
            cost_estimate=pl.CostEstimate(
                flops=2 * NM * TOK * D * FF,
                bytes_accessed=2 * NM * (TOK * (D + FF) + D * FF),
                transcendentals=0,
            ),
        )(a, g)
        return out

    return jax.shard_map(
        body, mesh=mesh, in_specs=(P(("rep", "dp")), P(("rep", "dp"))),
        out_specs=P("rep"), check_vma=False,
    )
```

```python
import functools

import jax
import jax.numpy as jnp
from jax import lax
from jax.experimental import pallas as pl
from jax.experimental.pallas import tpu as pltpu
from jax.sharding import PartitionSpec as P

MESH = pl.DeviceIdType.MESH
NM, TOK, D, FF = 4, 4096, 1536, 4224
HALF = D // 2
TM, TN, UM = 256, 1408, 128
TILES, SLICES = HALF // TM, FF // TN
CHUNKS = NM * SLICES * TILES
UPC = TM // UM
U = CHUNKS * UPC
STEPS = 2 * CHUNKS
GSTEPS = 2 * TILES
GROUPS = NM * SLICES
TREES = (
    (False, 1, 1), (True, 1, 0), (False, 2, 1), (False, 2, 0), (False, 1, 0), (True, 2, 0), (False, 1, 0), (True, 1, 0),
    (False, 2, 1), (False, 1, 1), (False, 2, 0), (False, 1, 1), (False, 1, 1), (False, 2, 1), (False, 1, 1), (False, 2, 0),
    (False, 1, 0), (False, 2, 1), (True, 0, 1), (False, 2, 0), (False, 1, 1), (False, 1, 0), (False, 1, 0), (True, 2, 1),
    (False, 1, 1), (False, 1, 1), (True, 3, 1), (True, 2, 1), (False, 1, 0), (False, 2, 1), (True, 3, 1), (True, 1, 0),
    (True, 0, 1), (False, 1, 0), (False, 2, 1), (True, 1, 0), (False, 1, 1), (True, 1, 1), (True, 2, 1), (True, 2, 1),
    (False, 1, 0), (True, 0, 0), (False, 1, 0), (True, 3, 1), (True, 1, 0), (False, 2, 0), (False, 1, 1), (True, 2, 1),
    (False, 2, 1), (True, 1, 1), (False, 1, 1), (False, 1, 0), (False, 1, 1), (False, 2, 0), (False, 1, 1), (False, 1, 0),
    (True, 3, 0), (False, 1, 0), (False, 2, 0), (False, 1, 1), (False, 2, 1), (False, 1, 1), (False, 1, 1), (False, 2, 0),
    (False, 1, 0), (False, 1, 0), (False, 1, 0), (False, 1, 1), (True, 2, 1), (False, 2, 1), (False, 1, 0), (False, 1, 1),
)
LAG_UP = (1, 5, 9, 13, 17)
LAG_DOWN = ((13, 19, 25, 31, 37), (17, 23, 29, 35, 41))
OB = 18
RC = 9
BR = 30
TOTAL = U + max(map(max, LAG_DOWN)) + 1
assert UPC == 2 and OB > LAG_UP[4] - LAG_UP[0] and 2 * RC > LAG_UP[4]
assert BR > max(map(max, LAG_DOWN)) - min(LAG_UP[3:])


def pick(values, i):
    out = jnp.int32(values[-1])
    for j in reversed(range(len(values) - 1)):
        out = jnp.where(i == j, values[j], out)
    return out


def bits(values, u):
    words = [
        sum(int(v) << j for j, v in enumerate(values[w : w + 24]))
        for w in range(0, U, 24)
    ]
    return (pick(words, u // 24) >> (u % 24)) & 1


def tree(u, y, z):
    kind_b = bits([t[0] for t in TREES], u) == 1
    k = bits([t[1] % 2 for t in TREES], u) + 2 * bits([t[1] // 2 for t in TREES], u)
    q = bits([t[2] for t in TREES], u)
    at_q = y == q
    on_line = kind_b | at_q
    at_k = z == k
    far = jnp.maximum(k, 3 - k)
    side = jnp.where(z < k, z, jnp.where(z > k, 3 - z, far))
    root = at_q & at_k
    height = jnp.where(
        kind_b, side + root.astype(jnp.int32), jnp.where(at_q, 1 + side, 0)
    )
    top = far + 1
    depth = jnp.abs(z - k) + (1 - at_q.astype(jnp.int32))
    child = (
        at_q & (at_k | ~kind_b),
        on_line & (z <= k) & (z > 0),
        on_line & (z >= k) & (z < 3),
    )
    parent = (
        ~at_q & (at_k | ~kind_b),
        on_line & (z > k),
        on_line & (z < k),
    )
    return height, top, depth, root, child, parent


def kernel(
    a_ref, g_ref, out_ref, box_ref,
    abuf, gbuf, sibout, own, outbox, stage,
    a_sem, g_sem, sib_send, recv, load, up_send, down_send, res, sibres,
):
    rep = lax.axis_index("rep")
    me = lax.axis_index("dp")
    core, z, y = me % 2, (me // 2) % 4, me // 8
    sib = (rep, me + 1 - 2 * core)
    near = (
        (rep, me + 8 - 16 * y),
        (rep, jnp.where(z > 0, me - 2, me + 2)),
        (rep, jnp.where(z < 3, me + 2, me - 2)),
    )

    def a_load(i):
        c = i // 2
        n, t = c // (SLICES * TILES), c % TILES
        half = jnp.where(i % 2 == 0, 1 - core, core)
        cols = pl.ds(pl.multiple_of(half * HALF + t * TM, 128), TM)
        return pltpu.make_async_copy(
            a_ref.at[0, n, :, cols], abuf.at[i % 2], a_sem.at[i % 2]
        )

    def g_load(gi):
        cols = pl.ds(pl.multiple_of((gi % SLICES) * TN, 128), TN)
        return pltpu.make_async_copy(
            g_ref.at[0, gi // SLICES, :, cols], gbuf.at[gi % 2], g_sem.at[gi % 2]
        )

    def remote(src, dst, send, rcv, device):
        return pltpu.make_async_remote_copy(
            src_ref=src, dst_ref=dst, send_sem=send, recv_sem=rcv,
            device_id=device, device_id_type=MESH,
        )

    def place(u):
        c = u // UPC
        n, s, t = c // (SLICES * TILES), (c // TILES) % SLICES, c % TILES
        row = pl.multiple_of(core * HALF + t * TM + (u % UPC) * UM, UM)
        col = pl.multiple_of(s * TN, 128)
        return out_ref.at[n, pl.ds(row, UM), pl.ds(col, TN)]

    def sib_copy(c, h):
        return remote(
            sibout.at[c % 2, pl.ds(h * UM, UM)], box_ref.at[c * UPC + h],
            sib_send.at[c % 2, h], recv.at[0, c * UPC + h], sib,
        )

    def up_copy(u, d):
        s = (1, 3, 2)[d]
        return remote(
            outbox.at[u % OB], box_ref.at[s * U + u], up_send.at[u % OB, 0],
            recv.at[s, u], near[d],
        )

    def root_copy(u, d):
        return remote(
            outbox.at[u % OB], place(u), up_send.at[u % OB, d],
            res.at[u], near[d],
        )

    def root_sib(u):
        return remote(
            outbox.at[u % OB], place(u), up_send.at[u % OB, 3], sibres.at[u], sib
        )

    def root_local(u):
        return pltpu.make_async_copy(
            outbox.at[u % OB], place(u), up_send.at[u % OB, 4]
        )

    def down_copy(u, d):
        return remote(place(u), place(u), down_send.at[u % BR, d], res.at[u], near[d])

    def down_sib(u):
        return remote(place(u), place(u), down_send.at[u % BR, 3], sibres.at[u], sib)

    def up_done(u):
        _, _, _, root, child, parent = tree(u, y, z)
        for d in range(3):
            @pl.when(parent[d])
            def _(d=d):
                up_copy(u, d).wait_send()

            @pl.when(root & child[d])
            def _(d=d):
                root_copy(u, d).wait_send()

        @pl.when(root)
        def _():
            root_sib(u).wait_send()
            root_local(u).wait()

    def down_done(u):
        _, _, _, root, child, _ = tree(u, y, z)
        for d in range(3):
            @pl.when(~root & child[d])
            def _(d=d):
                down_copy(u, d).wait_send()

        @pl.when(~root)
        def _():
            down_sib(u).wait_send()

    def stage_load(tau, u, s, slot):
        return pltpu.make_async_copy(
            box_ref.at[s * U + u], stage.at[tau, slot], load.at[tau, slot]
        )

    def gather(i):
        def one(tau, _):
            u = i - pick(LAG_UP, tau)
            ok = (u >= 0) & (u < U)
            uu = jnp.clip(u, 0, U - 1)
            height, _, _, _, child, _ = tree(uu, y, z)

            @pl.when(ok & (height == tau))
            def _():
                remote(box_ref.at[uu], box_ref.at[uu], sib_send.at[0, 0],
                       recv.at[0, uu], sib).wait_recv()
                stage_load(tau, uu, 0, 0).start()
                slot = jnp.int32(1)
                for d in range(3):
                    @pl.when(child[d])
                    def _(d=d, slot=slot):
                        b = box_ref.at[(d + 1) * U + uu]
                        remote(b, b, sib_send.at[0, 0], recv.at[d + 1, uu], sib).wait_recv()
                        stage_load(tau, uu, d + 1, slot).start()

                    slot = slot + child[d].astype(jnp.int32)

            return 0

        lax.fori_loop(0, 5, one, 0)

    def combine(i):
        def one(tau, _):
            u = i - pick(LAG_UP, tau)
            ok = (u >= 0) & (u < U)
            uu = jnp.clip(u, 0, U - 1)
            height, _, _, root, child, parent = tree(uu, y, z)
            count = sum(c.astype(jnp.int32) for c in child)

            @pl.when(ok & (height == tau))
            def _():
                @pl.when(uu >= OB)
                def _():
                    up_done(jnp.maximum(uu - OB, 0))

                for m in range(4):
                    @pl.when(count == m)
                    def _(m=m):
                        for slot in range(m + 1):
                            stage_load(tau, uu, 0, slot).wait()

                        def rows(r, _):
                            here = pl.ds(pl.multiple_of(r * 16, 16), 16)
                            there = pl.ds(
                                pl.multiple_of((uu % UPC) * UM + r * 16, 16), 16
                            )
                            acc = own[(uu // UPC) % RC, there, :]
                            for slot in range(m + 1):
                                acc = acc + stage[tau, slot, here, :].astype(jnp.float32)
                            outbox[uu % OB, here, :] = acc.astype(jnp.bfloat16)
                            return 0

                        lax.fori_loop(0, UM // 16, rows, 0)

                for d in range(3):
                    @pl.when(parent[d])
                    def _(d=d):
                        up_copy(uu, d).start()

                    @pl.when(root & child[d])
                    def _(d=d):
                        root_copy(uu, d).start()

                @pl.when(root)
                def _():
                    root_sib(uu).start()
                    root_local(uu).start()

            return 0

        lax.fori_loop(0, 5, one, 0)

    def forward(i):
        def one(tau, _):
            up, down = 3 + tau // 5, tau % 5
            u = i - pick(LAG_DOWN[0] + LAG_DOWN[1], tau)
            ok = (u >= 0) & (u < U)
            uu = jnp.clip(u, 0, U - 1)
            _, top, depth, root, child, _ = tree(uu, y, z)

            @pl.when(ok & (top == up) & (depth == down))
            def _():
                @pl.when(uu >= BR)
                def _():
                    down_done(jnp.maximum(uu - BR, 0))

                @pl.when(~root)
                def _():
                    remote(place(uu), place(uu), sib_send.at[0, 0], res.at[uu], sib).wait_recv()
                    for d in range(3):
                        @pl.when(child[d])
                        def _(d=d):
                            down_copy(uu, d).start()

                    down_sib(uu).start()

            return 0

        lax.fori_loop(0, 10, one, 0)

    def matmul(i):
        @pl.when(i % GSTEPS == 0)
        def _():
            g_load(i // GSTEPS).wait()

            @pl.when(i // GSTEPS + 1 < GROUPS)
            def _():
                g_load(i // GSTEPS + 1).start()

        a_load(i).wait()

        @pl.when(i + 1 < STEPS)
        def _():
            a_load(i + 1).start()

        c = i // 2

        def dot():
            return lax.dot_general(
                abuf[i % 2], gbuf[(i // GSTEPS) % 2], (((0,), (0,)), ((), ())),
                preferred_element_type=jnp.float32,
            )

        @pl.when(i % 2 == 0)
        def _():
            @pl.when(c >= 2)
            def _():
                for h in range(UPC):
                    sib_copy(jnp.maximum(c - 2, 0), h).wait_send()

            sibout[c % 2] = dot().astype(jnp.bfloat16)
            for h in range(UPC):
                sib_copy(c, h).start()

        @pl.when(i % 2 == 1)
        def _():
            own[c % RC] = dot()

    a_load(0).start()
    g_load(0).start()
    barrier = pltpu.get_barrier_semaphore()
    pl.semaphore_signal(barrier, inc=1, device_id=sib, device_id_type=MESH)
    pl.semaphore_signal(barrier, inc=1, device_id=near[0], device_id_type=MESH)

    @pl.when(z > 0)
    def _():
        pl.semaphore_signal(barrier, inc=1, device_id=near[1], device_id_type=MESH)

    @pl.when(z < 3)
    def _():
        pl.semaphore_signal(barrier, inc=1, device_id=near[2], device_id_type=MESH)

    inner = (z > 0) & (z < 3)

    @pl.when(inner)
    def _():
        pl.semaphore_wait(barrier, 4)

    @pl.when(~inner)
    def _():
        pl.semaphore_wait(barrier, 3)

    def step(i, _):
        forward(i)
        gather(i)

        @pl.when(i < STEPS)
        def _():
            matmul(i)

        combine(i)
        return 0

    lax.fori_loop(0, TOTAL, step, 0)

    for c in range(CHUNKS - 2, CHUNKS):
        for h in range(UPC):
            sib_copy(c, h).wait_send()

    def end_up(u, _):
        up_done(u)
        return 0

    lax.fori_loop(U - OB, U, end_up, 0)

    def end_down(u, _):
        down_done(u)
        return 0

    lax.fori_loop(U - BR, U, end_down, 0)

    def end_sib(u, _):
        c = u // UPC
        n, s, t = c // (SLICES * TILES), (c // TILES) % SLICES, c % TILES
        row = pl.multiple_of((1 - core) * HALF + t * TM + (u % UPC) * UM, UM)
        b = out_ref.at[n, pl.ds(row, UM), pl.ds(pl.multiple_of(s * TN, 128), TN)]
        remote(b, b, sib_send.at[0, 0], sibres.at[u], sib).wait_recv()
        return 0

    lax.fori_loop(0, U, end_sib, 0)


def solution(mesh):
    def body(a, g):
        dma = pltpu.SemaphoreType.DMA
        out, _ = pl.pallas_call(
            kernel,
            out_shape=[
                jax.ShapeDtypeStruct((NM, D, FF), jnp.bfloat16),
                jax.ShapeDtypeStruct((4 * U, UM, TN), jnp.bfloat16),
            ],
            in_specs=[pl.BlockSpec(memory_space=pl.ANY)] * 2,
            out_specs=[pl.BlockSpec(memory_space=pl.ANY)] * 2,
            scratch_shapes=[
                pltpu.VMEM((2, TOK, TM), jnp.bfloat16),
                pltpu.VMEM((2, TOK, TN), jnp.bfloat16),
                pltpu.VMEM((2, TM, TN), jnp.bfloat16),
                pltpu.VMEM((RC, TM, TN), jnp.float32),
                pltpu.VMEM((OB, UM, TN), jnp.bfloat16),
                pltpu.VMEM((5, 4, UM, TN), jnp.bfloat16),
                dma((2,)),
                dma((2,)),
                dma((2, UPC)),
                dma((4, U)),
                dma((5, 4)),
                dma((OB, 5)),
                dma((BR, 4)),
                dma((U,)),
                dma((U,)),
            ],
            compiler_params=pltpu.CompilerParams(
                collective_id=0, has_side_effects=True, vmem_limit_bytes=63 * 2**20
            ),
            cost_estimate=pl.CostEstimate(
                flops=2 * NM * TOK * D * FF,
                bytes_accessed=2 * NM * (TOK * (D + FF) + D * FF),
                transcendentals=0,
            ),
        )(a, g)
        return out

    return jax.shard_map(
        body, mesh=mesh, in_specs=(P(("rep", "dp")), P(("rep", "dp"))),
        out_specs=P("rep"), check_vma=False,
    )
```
